32 devices in a mesh: freq: 4 (over y, x), row: 8 (over z, core).
Axes of the slice: x: 2, y: 2, z: 4, core: 2. Of those that a mesh axis runs over, the one named last changes fastest.
Arguments:
- data: bfloat16 [4, 2, 2048, 2048], P('freq', None, 'row'), may hold values from -60 to 60
Outputs:
- solution: float32 [4, 2, 2048, 2048], P('freq', None, 'row')
- direction: float32 [4, 2, 2048, 2048], P('freq', None, 'row')
The draws below stay inside these ranges and needn't reach their ends.
All inputs are finite; a program needn't handle non-finite values.
Results may differ from the reference program's by a relative error of at most 0.0042.
Values may be sent and summed in bfloat16 or wider, within the bound.
A program may use at most 128 MiB of HBM per device.

```python
import math
import jax
import jax.numpy as jnp
from jax import lax

STATIONS = 2048
ITERS = 2
FREQS = 4


def draw_data(key, part):
    keys = jax.random.split(jax.random.fold_in(key, 11), 3)
    noise = jnp.clip(jax.random.normal(keys[0], (FREQS, 2, STATIONS, STATIONS), jnp.float32), -4.0, 4.0)
    rise_rows = 3.0 ** (jnp.arange(STATIONS, dtype=jnp.float32) / max(STATIONS - 1, 1) - 1.0)
    rise_freq = 3.0 ** (jnp.arange(FREQS, dtype=jnp.float32) / max(FREQS - 1, 1) - 1.0)
    jitter = jnp.exp(jax.random.uniform(keys[1], (FREQS, 1, STATIONS, 1), jnp.float32, math.log(0.7), math.log(1.4)))
    columns = jnp.exp(jax.random.uniform(keys[2], (FREQS, 1, 1, STATIONS), jnp.float32, math.log(0.5), math.log(2.0)))
    scaled = noise * jitter * columns * rise_rows[None, None, :, None] * rise_freq[:, None, None, None]
    return scaled.astype(jnp.bfloat16)


def setup_inputs(seed: int = 0) -> dict:
    key_list = jax.random.split(jax.random.key(seed), 2)
    data = draw_data(jax.random.fold_in(key_list[1], 71), 0)
    return dict(data=data)


def coupling():
    return 1.0 / (3.0 * (2.0 * STATIONS) ** 0.5)

def rounded_copy(field):
    rounded = lax.optimization_barrier(field.astype(jnp.bfloat16))
    return rounded.astype(jnp.float32)

def forward_map(field, data):
    rounded = rounded_copy(field)
    slices = data.astype(jnp.float32)
    best = lax.Precision.HIGHEST
    real_part = jnp.einsum('frk,fkn->frn', rounded[:, 0], slices[:, 0], precision=best) - jnp.einsum('frk,fkn->frn', rounded[:, 1], slices[:, 1], precision=best)
    imag_part = jnp.einsum('frk,fkn->frn', rounded[:, 0], slices[:, 1], precision=best) + jnp.einsum('frk,fkn->frn', rounded[:, 1], slices[:, 0], precision=best)
    return field - coupling() * jnp.stack([real_part, imag_part], axis=1)

def adjoint_map(field, data):
    rounded = rounded_copy(field)
    slices = data.astype(jnp.float32)
    best = lax.Precision.HIGHEST
    real_part = jnp.einsum('frk,fnk->frn', rounded[:, 0], slices[:, 0], precision=best) + jnp.einsum('frk,fnk->frn', rounded[:, 1], slices[:, 1], precision=best)
    imag_part = jnp.einsum('frk,fnk->frn', rounded[:, 1], slices[:, 0], precision=best) - jnp.einsum('frk,fnk->frn', rounded[:, 0], slices[:, 1], precision=best)
    return field - coupling() * jnp.stack([real_part, imag_part], axis=1)

def pair_step(data_raw, model_unit, data):
    beta_now = jnp.sqrt(jnp.sum(data_raw * data_raw))
    image = adjoint_map(data_raw, data)
    model_raw = image / beta_now - beta_now * model_unit
    alpha_now = jnp.sqrt(jnp.sum(model_raw * model_raw))
    return (beta_now, data_raw / beta_now, model_raw, alpha_now, model_raw / alpha_now)

def reference(data):
    observed = data.astype(jnp.float32)
    zeros = jnp.zeros_like(observed)
    beta_now, data_unit, model_raw, alpha_now, model_unit = pair_step(observed, zeros, data)
    solution = zeros
    direction = model_unit
    phi_bar = beta_now
    rho_bar = alpha_now
    for iteration in range(ITERS):
        data_raw = forward_map(model_raw, data) / alpha_now - alpha_now * data_unit
        beta_now, data_unit, model_raw, alpha_now, model_unit = pair_step(data_raw, model_unit, data)
        rho_value = jnp.sqrt(rho_bar * rho_bar + beta_now * beta_now)
        cosine = rho_bar / rho_value
        sine_value = beta_now / rho_value
        theta_value = sine_value * alpha_now
        rho_bar = -cosine * alpha_now
        phi_value = cosine * phi_bar
        phi_bar = sine_value * phi_bar
        solution = solution + phi_value / rho_value * direction
        direction = model_unit - theta_value / rho_value * direction
    return (solution, direction)
```

```python
import functools

import jax
import jax.numpy as jnp
from jax import lax
from jax.experimental import pallas as pl
from jax.experimental.pallas import tpu as pltpu
from jax.sharding import PartitionSpec as P

ITERS = 2
MESH = pl.DeviceIdType.MESH
F32 = jnp.float32
BF16 = jnp.bfloat16


def dot(a, b):
    return lax.dot_general(a, b, (((1,), (0,)), ((), ())), preferred_element_type=F32)


def dot_t(a, b):
    return lax.dot_general(a, b, (((1,), (1,)), ((), ())), preferred_element_type=F32)


def lane_sums(x):
    s = jnp.sum(x, axis=0, keepdims=True)
    return functools.reduce(jnp.add, [s[:, i : i + 128] for i in range(0, s.shape[1], 128)])


def kernel(
    n, nf, weight, data, sol_out, dir_out,
    full, va, vd, d_raw, m_raw, image, direc, work, stats, slots, sums, fslots,
    load_sem, ssem, rsem, st_s, st_r, sf_s, sf_r, out_sem,
):
    rows, order = data.shape[2], data.shape[3]
    m = n // 2
    me = lax.axis_index("row")
    mf = lax.axis_index("freq")
    z, c = lax.div(me, 2), lax.rem(me, 2)
    overlap = rows % 128 == 0
    unit = rows if overlap else min(order, 256)
    wide = min(order, 512)

    def at_row(r):
        return {"row": r}

    def piece(zb, cc, p):
        start = pl.multiple_of((zb * 2 + cc) * rows, rows)
        return full.at[p, pl.ds(start, rows), :]

    loads = []
    for p in range(2):
        loads.append(pltpu.make_async_copy(data.at[0, p], piece(z, c, p), load_sem.at[p]))
        loads.append(
            pltpu.make_async_copy(
                data.at[0, p], vd.at[pl.ds(p * rows, rows), :], load_sem.at[2 + p]
            )
        )
    for copy in loads:
        copy.start()

    barrier = pltpu.get_barrier_semaphore()

    @pl.loop(1, n)
    def _(k):
        pl.semaphore_signal(
            barrier, inc=1, device_id=at_row(lax.rem(me + k, n)), device_id_type=MESH
        )

    @pl.loop(1, nf)
    def _(k):
        pl.semaphore_signal(
            barrier, inc=1, device_id={"freq": lax.rem(mf + k, nf)}, device_id_type=MESH
        )

    for copy in loads:
        copy.wait()

    stats[...] = jnp.zeros_like(stats)

    @pl.loop(0, order // wide)
    def _(i):
        x = vd[:, pl.ds(pl.multiple_of(i * wide, wide), wide)].astype(F32)
        stats[0, 0:1, :] += lane_sums(x * x)

    pl.semaphore_wait(barrier, n - 1 + nf - 1)

    def row_stat(k, j):
        return pltpu.make_async_remote_copy(
            src_ref=stats.at[k], dst_ref=slots.at[k, me], send_sem=st_s.at[k, j],
            recv_sem=st_r.at[k, me], device_id=at_row(j), device_id_type=MESH,
        )

    def row_arrival(k, j):
        return pltpu.make_async_remote_copy(
            src_ref=stats.at[k], dst_ref=slots.at[k, j], send_sem=st_s.at[k, j],
            recv_sem=st_r.at[k, j], device_id=at_row(j), device_id_type=MESH,
        )

    def freq_stat(k, j):
        return pltpu.make_async_remote_copy(
            src_ref=sums.at[k], dst_ref=fslots.at[k, mf], send_sem=sf_s.at[k, j],
            recv_sem=sf_r.at[k, mf], device_id={"freq": j}, device_id_type=MESH,
        )

    def freq_arrival(k, j):
        return pltpu.make_async_remote_copy(
            src_ref=sums.at[k], dst_ref=fslots.at[k, j], send_sem=sf_s.at[k, j],
            recv_sem=sf_r.at[k, j], device_id={"freq": j}, device_id_type=MESH,
        )

    def start_sum(k):
        slots[k, me] = stats[k]

        @pl.loop(1, n)
        def _(i):
            row_stat(k, lax.rem(me + i, n)).start()

    def finish_sum(k):
        @pl.loop(1, n)
        def _(i):
            row_arrival(k, lax.rem(me + i, n)).wait_recv()

        total = lax.fori_loop(
            1, n, lambda j, t: t + slots[k, j], slots[k, 0]
        )
        sums[k] = total
        fslots[k, mf] = total

        @pl.loop(1, nf)
        def _(i):
            freq_stat(k, lax.rem(mf + i, nf)).start()

        @pl.loop(1, nf)
        def _(i):
            freq_arrival(k, lax.rem(mf + i, nf)).wait_recv()

        total = lax.fori_loop(
            1, nf, lambda j, t: t + fslots[k, j], fslots[k, 0]
        )
        values = jnp.sum(total, axis=1, keepdims=True)
        return [values[q : q + 1, :] for q in range(4)]

    def drain_sum(k):
        @pl.loop(1, n)
        def _(i):
            row_stat(k, lax.rem(me + i, n)).wait_send()

        @pl.loop(1, nf)
        def _(i):
            freq_stat(k, lax.rem(mf + i, nf)).wait_send()

    def block_copy(lane, zb, cc, p, target):
        return pltpu.make_async_remote_copy(
            src_ref=piece(zb, cc, p), dst_ref=piece(zb, cc, p),
            send_sem=ssem.at[lane, zb, p], recv_sem=rsem.at[zb * 2 + cc, p],
            device_id=at_row(target), device_id_type=MESH,
        )

    sibling = z * 2 + (1 - c)

    def spread(zb, p, below, above):
        @pl.when(below & (z + 1 < m))
        def _():
            block_copy(0, zb, c, p, lax.rem(me + 2, n)).start()

        @pl.when(above & (z > 0))
        def _():
            block_copy(1, zb, c, p, lax.rem(me + n - 2, n)).start()

        block_copy(2, zb, c, p, sibling).start()

    def settle(zb, p):
        @pl.when((zb <= z) & (z + 1 < m))
        def _():
            block_copy(0, zb, c, p, lax.rem(me + 2, n)).wait_send()

        @pl.when((zb >= z) & (z > 0))
        def _():
            block_copy(1, zb, c, p, lax.rem(me + n - 2, n)).wait_send()

        block_copy(2, zb, c, p, sibling).wait_send()

    start_sum(0)
    yes = m > 0
    for p in range(2):
        spread(z, p, jnp.bool_(yes), jnp.bool_(yes))

    @pl.loop(0, order // wide)
    def _(i):
        cols = pl.ds(pl.multiple_of(i * wide, wide), wide)
        work[:, cols] = jnp.zeros((2 * rows, wide), F32)

    beta = jnp.sqrt(finish_sum(0)[0])

    def process(start):
        band = pl.ds(pl.multiple_of(start, unit), unit)
        tr = dot_t(vd[...], full[0, band, :])
        ti = dot_t(vd[...], full[1, band, :])
        fit = jnp.concatenate([tr[:rows] + ti[rows:], tr[rows:] - ti[:rows]], axis=0)
        raw = (vd[:, band].astype(F32) - weight * fit) / beta
        m_raw[:, band] = raw
        stats[1, 0:1, :] += lane_sums(raw * raw)
        va[:, band] = raw.astype(BF16)

        @pl.loop(0, order // wide)
        def _(i):
            cols = pl.ds(pl.multiple_of(i * wide, wide), wide)
            v = va[:, band]
            a = dot(v, full[0, band, cols])
            b = dot(v, full[1, band, cols])
            work[:, cols] += jnp.concatenate(
                [a[:rows] - b[rows:], a[rows:] + b[:rows]], axis=0
            )

    @pl.loop(0, m)
    def _(s):
        @pl.when(s > 0)
        def _():
            for p in range(2):
                @pl.when(z - s >= 0)
                def _():
                    block_copy(0, z - s, c, p, sibling).wait_recv()
                    spread(z - s, p, jnp.bool_(True), jnp.bool_(False))

                @pl.when(z + s < m)
                def _():
                    block_copy(0, z + s, c, p, sibling).wait_recv()
                    spread(z + s, p, jnp.bool_(False), jnp.bool_(True))

        @pl.loop(0, 4)
        def _(t):
            up = lax.div(t, 2)
            other = lax.rem(t, 2)
            zb = z - s + 2 * s * up
            cc = c + other * (1 - 2 * c)

            @pl.when((zb >= 0) & (zb < m) & ((s > 0) | (t < 2)))
            def _():
                @pl.when(other == 1)
                def _():
                    for p in range(2):
                        block_copy(0, zb, cc, p, sibling).wait_recv()

                if overlap:
                    process((zb * 2 + cc) * rows)

    if not overlap:
        @pl.loop(0, order // unit)
        def _(u):
            process(u * unit)

    start_sum(1)
    alpha = jnp.sqrt(finish_sum(1)[0])

    chunk = min(order, 256)
    phi_bar, rho_bar = beta, alpha
    for it in range(ITERS):
        k = 2 + it
        inv_alpha, keep = 1.0 / alpha, alpha / beta

        @pl.loop(0, order // wide)
        def _(i):
            cols = pl.ds(pl.multiple_of(i * wide, wide), wide)
            if it == 0:
                fit = work[:, cols]
                old = vd[:, cols].astype(F32)
            else:
                a = dot(va[...], full[0, :, cols])
                b = dot(va[...], full[1, :, cols])
                fit = jnp.concatenate([a[:rows] - b[rows:], a[rows:] + b[:rows]], axis=0)
                old = d_raw[:, cols]
            model = m_raw[:, cols]
            new = (model - weight * fit) * inv_alpha - keep * old
            d_raw[:, cols] = new
            vd[:, cols] = new.astype(BF16)
            stats[k, 0:1, :] += lane_sums(new * new)
            stats[k, 3:4, :] += lane_sums(model * model)

        @pl.loop(0, order // wide)
        def _(i):
            cols = pl.ds(pl.multiple_of(i * wide, wide), wide)
            tr = dot_t(vd[...], full[0, cols, :])
            ti = dot_t(vd[...], full[1, cols, :])
            fit = jnp.concatenate([tr[:rows] + ti[rows:], tr[rows:] - ti[:rows]], axis=0)
            new = d_raw[:, cols] - weight * fit
            image[:, cols] = new
            stats[k, 1:2, :] += lane_sums(new * new)
            stats[k, 2:3, :] += lane_sums(new * m_raw[:, cols])

        start_sum(k)
        data_sq, image_sq, cross, model_sq = finish_sum(k)
        old_alpha = alpha
        beta = jnp.sqrt(data_sq)
        alpha = jnp.sqrt(
            image_sq / data_sq
            - 2.0 * cross / old_alpha
            + data_sq * (model_sq / (old_alpha * old_alpha))
        )
        rho = jnp.sqrt(rho_bar * rho_bar + beta * beta)
        cosine, sine = rho_bar / rho, beta / rho
        rho_bar = -cosine * alpha
        step = cosine * phi_bar / rho
        phi_bar = sine * phi_bar
        turn = sine * alpha / rho
        inv_beta, shift = 1.0 / beta, beta / old_alpha
        new_inv = 1.0 / alpha
        old_inv = 1.0 / old_alpha
        last = it == ITERS - 1

        tall = 2 * rows // 4 if rows % 16 == 0 else 2 * rows

        def leave(i, which):
            src, dst = (work, sol_out) if which == 0 else (direc, dir_out)
            per = rows // tall if tall <= rows else 1
            return pltpu.make_async_copy(
                src.at[pl.ds(pl.multiple_of(i * tall, tall), tall), :],
                dst.at[0, lax.div(i, per), pl.ds(pl.multiple_of(lax.rem(i, per) * tall, tall), tall), :],
                out_sem.at[which, i],
            )

        @pl.loop(0, 2 * rows // tall)
        def _(i):
            here = pl.ds(pl.multiple_of(i * tall, tall), tall)

            @pl.loop(0, order // chunk)
            def _(j):
                cols = pl.ds(pl.multiple_of(j * chunk, chunk), chunk)
                model = m_raw[here, cols]
                new = image[here, cols] * inv_beta - shift * model
                if it == 0:
                    old = model * old_inv
                    work[here, cols] = step * old
                else:
                    old = direc[here, cols]
                    work[here, cols] = work[here, cols] + step * old
                direc[here, cols] = new * new_inv - turn * old
                if not last:
                    m_raw[here, cols] = new
                    va[here, cols] = new.astype(BF16)

            if last:
                leave(i, 0).start()
                leave(i, 1).start()

    for k in range(2 + ITERS):
        drain_sum(k)

    @pl.loop(0, m)
    def _(zb):
        for p in range(2):
            settle(zb, p)

    @pl.loop(0, 2 * rows // tall)
    def _(i):
        leave(i, 0).wait()
        leave(i, 1).wait()


def on_device(n, nf, data):
    rows, order = data.shape[2], data.shape[3]
    weight = 1.0 / (3.0 * (2.0 * order) ** 0.5)
    field = pltpu.VMEM((2 * rows, order), F32)
    rounded = pltpu.VMEM((2 * rows, order), BF16)
    rounds = 2 + ITERS
    dma = pltpu.SemaphoreType.DMA
    out = jax.ShapeDtypeStruct(data.shape, F32)
    anywhere = pl.BlockSpec(memory_space=pl.ANY)
    return pl.pallas_call(
        functools.partial(kernel, n, nf, weight),
        out_shape=(out, out),
        in_specs=[anywhere],
        out_specs=(anywhere, anywhere),
        scratch_shapes=[
            pltpu.VMEM((2, order, order), BF16),
            rounded, rounded, field, field, field, field, field,
            pltpu.VMEM((rounds, 8, 128), F32),
            pltpu.VMEM((rounds, n, 8, 128), F32),
            pltpu.VMEM((rounds, 8, 128), F32),
            pltpu.VMEM((rounds, nf, 8, 128), F32),
            dma((4,)), dma((3, n // 2, 2)), dma((n, 2)),
            dma((rounds, n)), dma((rounds, n)),
            dma((rounds, nf)), dma((rounds, nf)),
            dma((2, 4)),
        ],
        compiler_params=pltpu.CompilerParams(
            collective_id=0, has_side_effects=True, vmem_limit_bytes=60 * 2**20
        ),
    )(data)


def solution(mesh):
    spec = P("freq", None, "row", None)
    return jax.shard_map(
        functools.partial(on_device, mesh.shape["row"], mesh.shape["freq"]),
        mesh=mesh,
        in_specs=(spec,),
        out_specs=(spec, spec),
        check_vma=False,
    )
```

```python
import functools

import jax
import jax.numpy as jnp
from jax import lax
from jax.experimental import pallas as pl
from jax.experimental.pallas import tpu as pltpu
from jax.sharding import PartitionSpec as P

ITERS = 2
MESH = pl.DeviceIdType.MESH
F32 = jnp.float32
BF16 = jnp.bfloat16


def dot(a, b):
    return lax.dot_general(a, b, (((1,), (0,)), ((), ())), preferred_element_type=F32)


def dot_t(a, b):
    return lax.dot_general(a, b, (((1,), (1,)), ((), ())), preferred_element_type=F32)


def lane_sums(x):
    s = jnp.sum(x, axis=0, keepdims=True)
    return functools.reduce(jnp.add, [s[:, i : i + 128] for i in range(0, s.shape[1], 128)])


def kernel(
    n, nf, weight, data, *refs,
):
    outs, refs = refs[: ITERS + 1], refs[ITERS + 1 :]
    coef, refs = refs[0], refs[1:]
    models, refs = refs[:ITERS], refs[ITERS:]
    (
        full, va, vd, d_raw, image, work, stats, slots, sums, fslots,
        load_sem, ssem, rsem, st_s, st_r, sf_s, sf_r, model_sem, image_sem,
    ) = refs
    m_raw = models[0]
    rows, order = data.shape[2], data.shape[3]
    m = n // 2
    me = lax.axis_index("row")
    mf = lax.axis_index("freq")
    z, c = lax.div(me, 2), lax.rem(me, 2)
    overlap = rows % 128 == 0
    unit = rows if overlap else min(order, 256)
    wide = min(order // 2, 512)

    def at_row(r):
        return {"row": r}

    def halves(body, between):
        count = order // wide
        pl.loop(0, count // 2)(body)
        between()
        pl.loop(count // 2, count)(body)

    def leave_model(it, p):
        return pltpu.make_async_copy(
            models[it].at[pl.ds(p * rows, rows), :], outs[it].at[0, p], model_sem.at[it, p]
        )

    def leave_image(i, p):
        cols = pl.ds(pl.multiple_of(i * wide, wide), wide)
        return pltpu.make_async_copy(
            image.at[pl.ds(p * rows, rows), cols],
            outs[ITERS].at[0, p, :, cols],
            image_sem.at[i, p],
        )

    def piece(zb, cc, p):
        start = pl.multiple_of((zb * 2 + cc) * rows, rows)
        return full.at[p, pl.ds(start, rows), :]

    loads = []
    for p in range(2):
        loads.append(pltpu.make_async_copy(data.at[0, p], piece(z, c, p), load_sem.at[p]))
        loads.append(
            pltpu.make_async_copy(
                data.at[0, p], vd.at[pl.ds(p * rows, rows), :], load_sem.at[2 + p]
            )
        )
    for copy in loads:
        copy.start()

    barrier = pltpu.get_barrier_semaphore()

    @pl.loop(1, n)
    def _(k):
        pl.semaphore_signal(
            barrier, inc=1, device_id=at_row(lax.rem(me + k, n)), device_id_type=MESH
        )

    @pl.loop(1, nf)
    def _(k):
        pl.semaphore_signal(
            barrier, inc=1, device_id={"freq": lax.rem(mf + k, nf)}, device_id_type=MESH
        )

    for copy in loads:
        copy.wait()

    stats[...] = jnp.zeros_like(stats)
    pl.semaphore_wait(barrier, n - 1 + nf - 1)

    def row_stat(k, j):
        return pltpu.make_async_remote_copy(
            src_ref=stats.at[k], dst_ref=slots.at[k, me], send_sem=st_s.at[k, j],
            recv_sem=st_r.at[k, me], device_id=at_row(j), device_id_type=MESH,
        )

    def row_arrival(k, j):
        return pltpu.make_async_remote_copy(
            src_ref=stats.at[k], dst_ref=slots.at[k, j], send_sem=st_s.at[k, j],
            recv_sem=st_r.at[k, j], device_id=at_row(j), device_id_type=MESH,
        )

    def freq_stat(k, j):
        return pltpu.make_async_remote_copy(
            src_ref=sums.at[k], dst_ref=fslots.at[k, mf], send_sem=sf_s.at[k, j],
            recv_sem=sf_r.at[k, mf], device_id={"freq": j}, device_id_type=MESH,
        )

    def freq_arrival(k, j):
        return pltpu.make_async_remote_copy(
            src_ref=sums.at[k], dst_ref=fslots.at[k, j], send_sem=sf_s.at[k, j],
            recv_sem=sf_r.at[k, j], device_id={"freq": j}, device_id_type=MESH,
        )

    def start_sum(k):
        slots[k, me] = stats[k]

        @pl.loop(1, n)
        def _(i):
            row_stat(k, lax.rem(me + i, n)).start()

    def middle_sum(k):
        @pl.loop(1, n)
        def _(i):
            row_arrival(k, lax.rem(me + i, n)).wait_recv()

        total = lax.fori_loop(
            1, n, lambda j, t: t + slots[k, j], slots[k, 0]
        )
        sums[k] = total
        fslots[k, mf] = total

        @pl.loop(1, nf)
        def _(i):
            freq_stat(k, lax.rem(mf + i, nf)).start()

    def finish_sum(k):
        @pl.loop(1, nf)
        def _(i):
            freq_arrival(k, lax.rem(mf + i, nf)).wait_recv()

        total = lax.fori_loop(
            1, nf, lambda j, t: t + fslots[k, j], fslots[k, 0]
        )
        values = jnp.sum(total, axis=1, keepdims=True)
        return [values[q : q + 1, :] for q in range(4)]

    def drain_sum(k):
        @pl.loop(1, n)
        def _(i):
            row_stat(k, lax.rem(me + i, n)).wait_send()

        @pl.loop(1, nf)
        def _(i):
            freq_stat(k, lax.rem(mf + i, nf)).wait_send()

    def block_copy(lane, zb, cc, p, target):
        return pltpu.make_async_remote_copy(
            src_ref=piece(zb, cc, p), dst_ref=piece(zb, cc, p),
            send_sem=ssem.at[lane, zb, p], recv_sem=rsem.at[zb * 2 + cc, p],
            device_id=at_row(target), device_id_type=MESH,
        )

    sibling = z * 2 + (1 - c)

    def spread(zb, p, below, above):
        @pl.when(below & (z + 1 < m))
        def _():
            block_copy(0, zb, c, p, lax.rem(me + 2, n)).start()

        @pl.when(above & (z > 0))
        def _():
            block_copy(1, zb, c, p, lax.rem(me + n - 2, n)).start()

        block_copy(2, zb, c, p, sibling).start()

    def settle(zb, p):
        @pl.when((zb <= z) & (z + 1 < m))
        def _():
            block_copy(0, zb, c, p, lax.rem(me + 2, n)).wait_send()

        @pl.when((zb >= z) & (z > 0))
        def _():
            block_copy(1, zb, c, p, lax.rem(me + n - 2, n)).wait_send()

        block_copy(2, zb, c, p, sibling).wait_send()

    spread(z, 0, jnp.bool_(True), jnp.bool_(True))

    @pl.loop(0, order // wide)
    def _(i):
        x = vd[:, pl.ds(pl.multiple_of(i * wide, wide), wide)].astype(F32)
        stats[0, 0:1, :] += lane_sums(x * x)

    start_sum(0)
    spread(z, 1, jnp.bool_(True), jnp.bool_(True))

    @pl.loop(0, order // wide)
    def _(i):
        cols = pl.ds(pl.multiple_of(i * wide, wide), wide)
        work[:, cols] = jnp.zeros((2 * rows, wide), F32)

    middle_sum(0)
    beta = jnp.sqrt(finish_sum(0)[0])

    def process(start):
        band = pl.ds(pl.multiple_of(start, unit), unit)
        tr = dot_t(vd[...], full[0, band, :])
        ti = dot_t(vd[...], full[1, band, :])
        fit = jnp.concatenate([tr[:rows] + ti[rows:], tr[rows:] - ti[:rows]], axis=0)
        raw = (vd[:, band].astype(F32) - weight * fit) / beta
        m_raw[:, band] = raw
        stats[1, 0:1, :] += lane_sums(raw * raw)
        va[:, band] = raw.astype(BF16)

        @pl.loop(0, order // wide)
        def _(i):
            cols = pl.ds(pl.multiple_of(i * wide, wide), wide)
            v = va[:, band]
            a = dot(v, full[0, band, cols])
            b = dot(v, full[1, band, cols])
            work[:, cols] += jnp.concatenate(
                [a[:rows] - b[rows:], a[rows:] + b[:rows]], axis=0
            )

    @pl.loop(0, m)
    def _(s):
        @pl.when(s > 0)
        def _():
            for p in range(2):
                @pl.when(z - s >= 0)
                def _():
                    block_copy(0, z - s, c, p, sibling).wait_recv()
                    spread(z - s, p, jnp.bool_(True), jnp.bool_(False))

                @pl.when(z + s < m)
                def _():
                    block_copy(0, z + s, c, p, sibling).wait_recv()
                    spread(z + s, p, jnp.bool_(False), jnp.bool_(True))

        @pl.loop(0, 4)
        def _(t):
            up = lax.div(t, 2)
            other = lax.rem(t, 2)
            zb = z - s + 2 * s * up
            cc = c + other * (1 - 2 * c)

            @pl.when((zb >= 0) & (zb < m) & ((s > 0) | (t < 2)))
            def _():
                @pl.when(other == 1)
                def _():
                    for p in range(2):
                        block_copy(0, zb, cc, p, sibling).wait_recv()

                if overlap:
                    process((zb * 2 + cc) * rows)

    if not overlap:
        @pl.loop(0, order // unit)
        def _(u):
            process(u * unit)

    start_sum(1)
    for p in range(2):
        leave_model(0, p).start()
    middle_sum(1)
    alpha = jnp.sqrt(finish_sum(1)[0])

    phi_bar, rho_bar = beta, alpha
    direction, answer = [1.0 / alpha], []
    for it in range(ITERS):
        last = it == ITERS - 1
        model_ref = models[it]
        ka, kb = 2 * it + 1, 2 * it + 2

        if it > 0:
            def forward(i):
                cols = pl.ds(pl.multiple_of(i * wide, wide), wide)
                a = dot(va[...], full[0, :, cols])
                b = dot(va[...], full[1, :, cols])
                work[:, cols] = jnp.concatenate(
                    [a[:rows] - b[rows:], a[rows:] + b[:rows]], axis=0
                )

            halves(forward, lambda: middle_sum(ka))
            alpha = jnp.sqrt(finish_sum(ka)[0])
            rotate(alpha)
        inv_alpha, keep = 1.0 / alpha, alpha / beta

        @pl.loop(0, order // wide)
        def _(i):
            cols = pl.ds(pl.multiple_of(i * wide, wide), wide)
            old = vd[:, cols].astype(F32) if it == 0 else d_raw[:, cols]
            new = (model_ref[:, cols] - weight * work[:, cols]) * inv_alpha - keep * old
            d_raw[:, cols] = new
            vd[:, cols] = new.astype(BF16)
            stats[kb, 0:1, :] += lane_sums(new * new)

        start_sum(kb)

        def adjoint(i):
            cols = pl.ds(pl.multiple_of(i * wide, wide), wide)
            tr = dot_t(vd[...], full[0, cols, :])
            ti = dot_t(vd[...], full[1, cols, :])
            fit = jnp.concatenate([tr[:rows] + ti[rows:], tr[rows:] - ti[:rows]], axis=0)
            new = d_raw[:, cols] - weight * fit
            image[:, cols] = new
            if last:
                stats[kb + 1, 0:1, :] += lane_sums(new * new)
                stats[kb + 1, 1:2, :] += lane_sums(new * model_ref[:, cols])
                for p in range(2):
                    leave_image(i, p).start()

        halves(adjoint, lambda: middle_sum(kb))
        if last:
            start_sum(kb + 1)
        data_sq = finish_sum(kb)[0]
        beta = jnp.sqrt(data_sq)
        inv_beta, shift = 1.0 / beta, beta / alpha

        if not last:
            @pl.loop(0, order // wide)
            def _(i):
                cols = pl.ds(pl.multiple_of(i * wide, wide), wide)
                new = image[:, cols] * inv_beta - shift * model_ref[:, cols]
                models[it + 1][:, cols] = new
                va[:, cols] = new.astype(BF16)
                stats[kb + 1, 0:1, :] += lane_sums(new * new)

            start_sum(kb + 1)
            for p in range(2):
                leave_model(it + 1, p).start()

        rho = jnp.sqrt(rho_bar * rho_bar + beta * beta)
        cosine, sine = rho_bar / rho, beta / rho
        step = cosine * phi_bar / rho
        phi_bar = sine * phi_bar
        answer = [x + step * w for x, w in zip(answer + [0.0], direction)]

        def rotate(alpha, sine=sine, cosine=cosine, rho=rho):
            nonlocal rho_bar, direction
            rho_bar = -cosine * alpha
            turn = sine * alpha / rho
            direction = [-turn * w for w in direction] + [1.0 / alpha]

    middle_sum(kb + 1)
    image_sq, cross = finish_sum(kb + 1)[:2]
    new_alpha = jnp.sqrt(image_sq / data_sq - 2.0 * cross / alpha + data_sq)
    rotate(new_alpha)
    tip = direction.pop()
    direction[-1] = direction[-1] - tip * shift
    direction.append(tip * inv_beta)
    for q, value in enumerate(answer + direction):
        coef[q : q + 1, :] = jnp.broadcast_to(value, (1, 128))

    for k in range(2 + 2 * ITERS):
        drain_sum(k)

    @pl.loop(0, m)
    def _(zb):
        for p in range(2):
            settle(zb, p)

    for p in range(2):
        for it in range(ITERS):
            leave_model(it, p).wait()

        @pl.loop(0, order // wide)
        def _(i):
            leave_image(i, p).wait()


def on_device(n, nf, data):
    rows, order = data.shape[2], data.shape[3]
    weight = 1.0 / (3.0 * (2.0 * order) ** 0.5)
    field = pltpu.VMEM((2 * rows, order), F32)
    rounded = pltpu.VMEM((2 * rows, order), BF16)
    rounds = 2 + 2 * ITERS
    dma = pltpu.SemaphoreType.DMA
    out = jax.ShapeDtypeStruct(data.shape, F32)
    anywhere = pl.BlockSpec(memory_space=pl.ANY)
    *basis, coef = pl.pallas_call(
        functools.partial(kernel, n, nf, weight),
        out_shape=(out,) * (ITERS + 1) + (jax.ShapeDtypeStruct((2 * ITERS + 1, 128), F32),),
        in_specs=[anywhere],
        out_specs=(anywhere,) * (ITERS + 1) + (pl.BlockSpec(memory_space=pltpu.VMEM),),
        scratch_shapes=[field] * ITERS
        + [
            pltpu.VMEM((2, order, order), BF16),
            rounded, rounded, field, field, field,
            pltpu.VMEM((rounds, 8, 128), F32),
            pltpu.VMEM((rounds, n, 8, 128), F32),
            pltpu.VMEM((rounds, 8, 128), F32),
            pltpu.VMEM((rounds, nf, 8, 128), F32),
            dma((4,)), dma((3, n // 2, 2)), dma((n, 2)),
            dma((rounds, n)), dma((rounds, n)),
            dma((rounds, nf)), dma((rounds, nf)),
            dma((ITERS, 2)), dma((max(2, order // 512), 2)),
        ],
        compiler_params=pltpu.CompilerParams(
            collective_id=0, has_side_effects=True, vmem_limit_bytes=60 * 2**20
        ),
    )(data)
    answer = sum(coef[k, 0] * basis[k] for k in range(ITERS))
    direction = sum(coef[ITERS + k, 0] * basis[k] for k in range(ITERS + 1))
    return answer, direction


def solution(mesh):
    spec = P("freq", None, "row", None)
    return jax.shard_map(
        functools.partial(on_device, mesh.shape["row"], mesh.shape["freq"]),
        mesh=mesh,
        in_specs=(spec,),
        out_specs=(spec, spec),
        check_vma=False,
    )
```
